32 devices in a mesh: region: 8 (over z, x), member: 4 (over y, core).
Axes of the slice: x: 2, y: 2, z: 4, core: 2. Of those that a mesh axis runs over, the one named last changes fastest.
Arguments:
- ensemble: bfloat16 [40, 131072], P('member', 'region'), may hold values from -6 to 6
- obs_value: float32 [1024, 128], P(('region', 'member')), may hold values from -8 to 8
- obs_var: float32 [1024, 128], P(('region', 'member')), may hold values from 0.1 to 1
- obs_point: int32 [1024, 128], P(('region', 'member')), may hold values from 0 to 16383
- owned_blocks: int32 [1024], P('region'), may hold values from 0 to 1023, each once
- infl_mean: float32 [1024], replicated, may hold values from 0.6 to 1.6
- infl_var: float32 [1024], replicated, may hold values from 0.0001 to 0.1
Outputs:
- inflated: bfloat16 [40, 131072], P('member', 'region')
- infl_post: float32 [1024], P(('region', 'member'))
The draws below stay inside these ranges and needn't reach their ends.
Inputs may be any that keep to these rules, and one draw needn't show every extreme that they name: `obs_point`: index among the 16384 points of the observation's region; the observation belongs to the block of that point's slot. `owned_blocks`: every block id appears exactly once.
All inputs are finite; a program needn't handle non-finite values.
Results may differ from the reference program's by a relative error of at most 0.001.
Values sent between devices are 32-bit elements; how exact they have to be, the bound alone decides.
A program may use at most 64 MiB of HBM per device.

```python
import math
import jax
import jax.numpy as jnp
from jax import lax

PTS_DEV = 16384
OBS_DEV = 4096
MEMBERS = 40
PTS = 131072
BLOCKS = 1024
SPAN = 128
OBS_ROWS = 1024
N_MEMBER = 4


def with_ends(values, rng, low, top_value):
    shape = values.shape
    index_at = [jax.random.randint(jax.random.fold_in(rng, axis), (), 0, shape[axis]) for axis in range(len(shape))]
    values = values.at[tuple(index_at)].set(low)
    longest = shape.index(max(shape))
    index_at[longest] = (index_at[longest] + 1) % shape[longest]
    return values.at[tuple(index_at)].set(top_value)


def block_scale(rng, shape, shards, least, largest):
    def one(position, shards_of):
        heights = jax.random.uniform(jax.random.fold_in(jax.random.fold_in(rng, 6), position), (shards_of,), jnp.float32, least / len(shards), largest / len(shards))
        return jnp.repeat(jnp.exp(heights), shape[position] // shards_of).reshape((-1,) + (1,) * (len(shape) - position - 1))

    loudness = one(*shards[0])
    for cut in shards[1:]:
        loudness = loudness * one(*cut)
    return loudness


def scatter_about(rng, extent, width, reach, shards=(), kind=jnp.bfloat16):
    gain = block_scale(rng, extent, shards, -0.22, 0.18) if shards else 1.0
    result = jax.random.normal(rng, extent, jnp.float32) * width * gain
    return jnp.minimum(jnp.maximum(result, -reach), reach).astype(kind)


def setup_inputs(seed: int = 0) -> dict:
    arg_keys = jax.random.split(jax.random.key(seed), 8)
    return {
        "ensemble": scatter_about(arg_keys[0], (MEMBERS, PTS), 1.0, 6.0, ((0, 4), (1, 8))),
        "obs_value": scatter_about(arg_keys[1], (OBS_ROWS, 128), 1.3, 8.0, ((0, 32),), jnp.float32),
        "obs_var": jnp.clip(jnp.exp(math.log(1.0) - 2.3025851 * jax.random.uniform(arg_keys[2], (OBS_ROWS, 128), jnp.float32) ** block_scale(arg_keys[2], (OBS_ROWS, 128), ((0, 32),), -0.2, 0.2)), 0.1, 1.0),
        "obs_point": with_ends(jax.random.randint(arg_keys[3], (OBS_ROWS, 128), 0, PTS_DEV), jax.random.fold_in(arg_keys[3], 1), 0, PTS_DEV - 1).astype(jnp.int32),
        "owned_blocks": jax.random.permutation(arg_keys[4], BLOCKS).astype(jnp.int32),
        "infl_mean": jnp.clip(jax.random.uniform(arg_keys[5], (BLOCKS,), jnp.float32, 0.6, 1.6), 0.6, 1.6),
        "infl_var": jnp.clip(jnp.exp(jax.random.uniform(arg_keys[6], (BLOCKS,), jnp.float32, math.log(0.0001), math.log(0.1))), 0.0001, 0.1),
    }


def posterior(sums, prior_mean, prior_var):
    innov_sum = sums[0]
    spread_sum = sums[1]
    error_sum = sums[2]
    spread_spread = sums[3]
    spread_error = sums[4]
    error_error = sums[5]
    weight_var = 2.0 * prior_mean * prior_mean * (1.0 + spread_spread) + 4.0 * prior_mean * spread_error + 2.0 * error_error
    value = (prior_mean * weight_var + prior_var * spread_sum * (innov_sum - error_sum)) / (weight_var + prior_var * spread_sum * spread_sum)
    return jnp.maximum(value, 1.0)

def reference(ensemble, obs_value, obs_var, obs_point, owned_blocks, infl_mean, infl_var):
    wide = ensemble.astype(jnp.float32)
    point_total = lax.optimization_barrier(jnp.sum(wide, 0))
    point_square = lax.optimization_barrier(jnp.sum(wide * wide, 0))
    point_mean = point_total / MEMBERS
    row_region = jnp.arange(OBS_ROWS, dtype=jnp.int32) // (OBS_DEV // 128 * N_MEMBER)
    global_point = (row_region[:, None] * PTS_DEV + obs_point).reshape(-1).astype(jnp.int32)
    at_mean = point_mean[global_point]
    at_square = point_square[global_point]
    spread = (at_square - MEMBERS * at_mean * at_mean) / (MEMBERS - 1)
    innovation = obs_value.reshape(-1) - at_mean
    errors = obs_var.reshape(-1)
    obs_blk = owned_blocks[(global_point // SPAN).astype(jnp.int32)].astype(jnp.int32)
    columns = jnp.stack([innovation * innovation, spread, errors, spread * spread, spread * errors, errors * errors], 1)
    sums = jax.ops.segment_sum(columns, obs_blk, num_segments=BLOCKS)
    infl_post = posterior(sums.T, infl_mean, infl_var)
    point_lambda = jnp.repeat(infl_post[owned_blocks], SPAN)
    inflated = (point_mean + jnp.sqrt(point_lambda) * (wide - point_mean)).astype(jnp.bfloat16)
    return (inflated, infl_post)
```

```python
import functools

import jax
import jax.numpy as jnp
from jax import lax
from jax.experimental import pallas as pl
from jax.experimental.pallas import tpu as pltpu
from jax.sharding import PartitionSpec as P

LANES = 128
MESH = pl.DeviceIdType.MESH
F32 = jnp.float32
BF16 = jnp.bfloat16
NT = (((1,), (1,)), ((), ()))


def split(value, parts):
    terms = []
    for _ in range(parts):
        term = value.astype(BF16).astype(F32)
        terms.append(term)
        value = value - term
    return terms


def to_row(table):
    slots = table.shape[0]
    eye = lax.broadcasted_iota(jnp.int32, (slots, slots), 0) == lax.broadcasted_iota(
        jnp.int32, (slots, slots), 1
    )
    column = jnp.sum(table, axis=1, keepdims=True)
    return jnp.sum(jnp.where(eye, column, 0.0), axis=0, keepdims=True)


def scatter(value_ref, var_ref, point_ref, acc, half):
    rows = point_ref.shape[0]
    step = 8
    planes = 10
    low_ids = lax.broadcasted_iota(jnp.int32, (half, LANES), 0)
    col_ids = lax.broadcasted_iota(jnp.int32, (2 * LANES, LANES), 0)

    def chunk(first):
        point = point_ref[pl.ds(first, step), :]
        slot = point >> 7
        upper = (slot >= half).astype(jnp.int32)
        low = slot - half * upper
        col = (point & (LANES - 1)) + LANES * upper
        y = split(value_ref[pl.ds(first, step), :], 2)
        exact = y[0] + y[1]
        v = var_ref[pl.ds(first, step), :]
        terms = [jnp.ones_like(v)] + y + split(exact * exact, 3) + split(v, 2) + split(v * v, 2)
        left, right = [], []
        for r in range(step):
            hot = (low_ids == low[r : r + 1, :]).astype(F32).astype(BF16)
            blocks = []
            for term in terms:
                wide = jnp.broadcast_to(term[r : r + 1, :], (16, LANES)).astype(BF16)
                blocks.append(hot * jnp.concatenate([wide] * (half // 16), 0))
            left.append(jnp.concatenate(blocks, 0))
            right.append((col_ids == col[r : r + 1, :]).astype(F32).astype(BF16))
        return lax.dot_general(
            jnp.concatenate(left, 1), jnp.concatenate(right, 1), NT, preferred_element_type=F32
        )

    acc[...] = chunk(0)

    @pl.loop(1, rows // step)
    def _(i):
        acc[...] += chunk(pl.multiple_of(i * step, step))

    def plane(i, j):
        part = acc[pl.ds(i * half, half), :]
        for other in range(i + 1, j):
            part = part + acc[pl.ds(other * half, half), :]
        return jnp.concatenate([part[:, :LANES], part[:, LANES:]], 0)

    return plane


def kernel(
    n_region, n_member, members,
    ens_hbm, value_hbm, var_hbm, point_hbm, owned_hbm, pmean_hbm, pvar_hbm,
    out_ref, post_ref,
    ens, value, var, point, owned, pmean, pvar,
    part, rs_recv, gathered, stats, factor, acc, place, place_recv,
    in_sem, rs_send, rs_got, ag_send, ag_got, st_send, st_got, pl_send, pl_got,
):
    region = lax.axis_index("region")
    me = lax.axis_index("member")
    slots = owned.shape[1]
    own = slots // n_member
    half = slots // 2

    barrier = pltpu.get_barrier_semaphore()
    for i in range(1, n_member):
        pl.semaphore_signal(
            barrier, inc=1, device_id={"member": lax.rem(me + i, n_member)}, device_id_type=MESH
        )
    for i in range(1, n_region):
        pl.semaphore_signal(
            barrier, inc=1, device_id={"region": lax.rem(region + i, n_region)}, device_id_type=MESH
        )
    pairs = (
        (ens_hbm, ens), (value_hbm, value), (var_hbm, var), (point_hbm, point),
        (owned_hbm, owned), (pmean_hbm, pmean), (pvar_hbm, pvar),
    )
    loads = [pltpu.make_async_copy(s, d, in_sem.at[i]) for i, (s, d) in enumerate(pairs)]
    for load in loads:
        load.start()

    loads[0].wait()

    @pl.loop(0, n_member)
    def _(k):
        @pl.loop(0, own, unroll=8)
        def _(r):
            start = pl.multiple_of((k * own + r) * LANES, LANES)
            wide = ens[:, pl.ds(start, LANES)].astype(F32)
            part[k, pl.ds(r, 1), :] = jnp.sum(wide, 0, keepdims=True)
            part[k, pl.ds(own + r, 1), :] = jnp.sum(wide * wide, 0, keepdims=True)

    pl.semaphore_wait(barrier, n_member + n_region - 2)
    rs = []
    for i in range(1, n_member):
        peer = lax.rem(me + i, n_member)
        copy = pltpu.make_async_remote_copy(
            part.at[peer], rs_recv.at[i], rs_send.at[i], rs_got.at[i],
            device_id={"member": peer}, device_id_type=MESH,
        )
        copy.start()
        rs.append(copy)

    for load in loads[1:]:
        load.wait()
    plane = scatter(value, var, point, acc, half)

    for copy in rs:
        copy.wait_recv()
    both = part[me]
    for i in range(1, n_member):
        both = both + rs_recv[i]
    mean_own = both[:own] / members
    gathered[me, :own, :] = mean_own
    gathered[me, own:, :] = (both[own:] - members * mean_own * mean_own) / (members - 1)
    ag = []
    for i in range(1, n_member):
        copy = pltpu.make_async_remote_copy(
            gathered.at[me], gathered.at[me], ag_send.at[i], ag_got.at[i],
            device_id={"member": lax.rem(me + i, n_member)}, device_id_type=MESH,
        )
        copy.start()
        ag.append(copy)

    block = owned[...]
    groups = pmean.shape[0]
    lane_hot = (
        lax.broadcasted_iota(jnp.int32, (LANES, slots), 0) == (block & (LANES - 1))
    ).astype(F32).astype(BF16)
    table = jnp.concatenate(split(pmean[...], 3) + split(pvar[...], 3), 0).astype(BF16)
    picked = jnp.dot(table, lane_hot, preferred_element_type=F32)
    in_group = lax.broadcasted_iota(jnp.int32, (groups, slots), 0) == (block >> 7)

    def pick(first):
        total = picked[first * groups : (first + 1) * groups]
        for i in (1, 2):
            total = total + picked[(first + i) * groups : (first + i + 1) * groups]
        return jnp.sum(jnp.where(in_group, total, 0.0), 0, keepdims=True)

    prior_mean, prior_var = pick(0), pick(3)
    count, y_sum, y_square, v_sum, v_square = (
        plane(0, 1), plane(1, 3), plane(3, 6), plane(6, 8), plane(8, 10)
    )
    error_sum = to_row(v_sum)
    error_error = to_row(v_square)

    for copy in ag:
        copy.wait_recv()
    mean = jnp.concatenate([gathered[k, :own, :] for k in range(n_member)], 0)
    spread = jnp.concatenate([gathered[k, own:, :] for k in range(n_member)], 0)
    seen = count * spread
    mine = jnp.concatenate(
        [
            to_row(y_square + mean * (count * mean - 2.0 * y_sum)),
            to_row(seen),
            error_sum,
            to_row(seen * spread),
            to_row(v_sum * spread),
            error_error,
            jnp.zeros((2, slots), F32),
        ],
        0,
    )
    stats[0] = mine
    st = []
    for i in range(1, n_member):
        copy = pltpu.make_async_remote_copy(
            stats.at[0], stats.at[i], st_send.at[i], st_got.at[i],
            device_id={"member": lax.rem(me + i, n_member)}, device_id_type=MESH,
        )
        copy.start()
        st.append(copy)
    for copy in st:
        copy.wait_recv()
    total = mine
    for i in range(1, n_member):
        total = total + stats[i]
    sd, sp, so = total[0:1], total[1:2], total[2:3]
    spp, spo, soo = total[3:4], total[4:5], total[5:6]
    weight = 2.0 * prior_mean * prior_mean * (1.0 + spp) + 4.0 * prior_mean * spo + 2.0 * soo
    post = jnp.maximum(
        (prior_mean * weight + prior_var * sp * (sd - so)) / (weight + prior_var * sp * sp), 1.0
    )

    share = groups * LANES // (n_region * n_member)
    holder = block // share
    to_me = lax.rem(holder, n_member) == me
    rows = max(8, n_region)
    target = lax.broadcasted_iota(jnp.int32, (rows, slots), 0) == jnp.where(
        to_me, holder // n_member, -1
    )
    spots = (
        lax.broadcasted_iota(jnp.int32, (LANES, slots), 0) == lax.rem(block, share)
    ).astype(F32).astype(BF16)
    sent = jnp.concatenate([jnp.where(target, term, 0.0) for term in split(post, 3)], 0)
    placed = lax.dot_general(sent.astype(BF16), spots, NT, preferred_element_type=F32)
    placed = placed[:rows] + placed[rows : 2 * rows] + placed[2 * rows :]
    for r in range(n_region):
        place[r] = placed[r : r + 1]
    out_copies = []
    for i in range(1, n_region):
        there = lax.rem(region + i, n_region)
        copy = pltpu.make_async_remote_copy(
            place.at[there], place_recv.at[i], pl_send.at[i], pl_got.at[i],
            device_id={"region": there}, device_id_type=MESH,
        )
        copy.start()
        out_copies.append(copy)

    eye = lax.broadcasted_iota(jnp.int32, (slots, slots), 0) == lax.broadcasted_iota(
        jnp.int32, (slots, slots), 1
    )
    column = jnp.sum(jnp.where(eye, post, 0.0), axis=1, keepdims=True)
    factor[...] = jnp.broadcast_to(jnp.sqrt(column), factor.shape)

    @pl.loop(0, n_member)
    def _(k):
        @pl.loop(0, own, unroll=8)
        def _(r):
            slot = k * own + r
            start = pl.multiple_of(slot * LANES, LANES)
            wide = ens[:, pl.ds(start, LANES)].astype(F32)
            at = gathered[k, pl.ds(r, 1), :]
            out_ref[:, pl.ds(start, LANES)] = (
                at + factor[pl.ds(slot, 1), :] * (wide - at)
            ).astype(BF16)

    for copy in out_copies:
        copy.wait_recv()
    result = place[region]
    for i in range(1, n_region):
        result = result + place_recv[i]
    post_ref[...] = result[:, :share]
    for copy in rs + ag + st + out_copies:
        copy.wait_send()


def body(n_region, n_member, ensemble, obs_value, obs_var, obs_point, owned, infl_mean, infl_var):
    members = ensemble.shape[0] * n_member
    slots = owned.shape[0]
    own = slots // n_member
    blocks = infl_mean.shape[0]
    share = blocks // (n_region * n_member)
    owned = owned.reshape(1, slots)
    infl_mean = infl_mean.reshape(-1, LANES)
    infl_var = infl_var.reshape(-1, LANES)
    operands = (ensemble, obs_value, obs_var, obs_point, owned, infl_mean, infl_var)
    dma = pltpu.SemaphoreType.DMA
    inflated, post = pl.pallas_call(
        functools.partial(kernel, n_region, n_member, members),
        out_shape=(
            jax.ShapeDtypeStruct(ensemble.shape, BF16),
            jax.ShapeDtypeStruct((1, share), F32),
        ),
        in_specs=[pl.BlockSpec(memory_space=pltpu.HBM)] * len(operands),
        out_specs=(
            pl.BlockSpec(memory_space=pltpu.VMEM),
            pl.BlockSpec(memory_space=pltpu.VMEM),
        ),
        scratch_shapes=[pltpu.VMEM(a.shape, a.dtype) for a in operands]
        + [
            pltpu.VMEM((n_member, 2 * own, LANES), F32),
            pltpu.VMEM((n_member, 2 * own, LANES), F32),
            pltpu.VMEM((n_member, 2 * own, LANES), F32),
            pltpu.VMEM((n_member, 8, slots), F32),
            pltpu.VMEM((slots, LANES), F32),
            pltpu.VMEM((10 * (slots // 2), 2 * LANES), F32),
            pltpu.VMEM((n_region, 1, LANES), F32),
            pltpu.VMEM((n_region, 1, LANES), F32),
            dma((len(operands),)),
            dma((n_member,)), dma((n_member,)),
            dma((n_member,)), dma((n_member,)),
            dma((n_member,)), dma((n_member,)),
            dma((n_region,)), dma((n_region,)),
        ],
        compiler_params=pltpu.CompilerParams(collective_id=0, has_side_effects=True),
    )(*operands)
    return inflated, post.reshape(share)


def solution(mesh):
    placed = (
        P("member", "region"),
        P(("region", "member"), None),
        P(("region", "member"), None),
        P(("region", "member"), None),
        P("region"),
        P(),
        P(),
    )
    return jax.shard_map(
        functools.partial(body, mesh.shape["region"], mesh.shape["member"]),
        mesh=mesh,
        in_specs=placed,
        out_specs=(P("member", "region"), P(("region", "member"))),
        check_vma=False,
    )
```

```python
import functools

import jax
import jax.numpy as jnp
from jax import lax
from jax.experimental import pallas as pl
from jax.experimental.pallas import tpu as pltpu
from jax.sharding import PartitionSpec as P

LANES = 128
MESH = pl.DeviceIdType.MESH
F32 = jnp.float32
BF16 = jnp.bfloat16
NT = (((1,), (1,)), ((), ()))


def split(value, parts):
    terms = []
    for _ in range(parts):
        term = value.astype(BF16).astype(F32)
        terms.append(term)
        value = value - term
    return terms


def scatter(value_ref, var_ref, point_ref, acc, row_acc, half):
    rows = point_ref.shape[0]
    step = 8
    low_ids = lax.broadcasted_iota(jnp.int32, (half, LANES), 0)
    col_ids = lax.broadcasted_iota(jnp.int32, (2 * LANES, LANES), 0)
    slot_ids = lax.broadcasted_iota(jnp.int32, (2 * half, LANES), 0)

    def chunk(first):
        point = point_ref[pl.ds(first, step), :]
        slot = point >> 7
        upper = (slot >= half).astype(jnp.int32)
        low = slot - half * upper
        col = (point & (LANES - 1)) + LANES * upper
        y = split(value_ref[pl.ds(first, step), :], 2)
        exact = y[0] + y[1]
        raw = var_ref[pl.ds(first, step), :]
        v = split(raw, 2)
        terms = [jnp.ones_like(raw)] + y + v
        row_terms = v + split(raw * raw, 3) + split(exact * exact, 3)
        left, right, hots = [], [], []
        row_left = []
        for r in range(step):
            here = slice(r, r + 1)
            hot = (low_ids == low[here, :]).astype(F32).astype(BF16)
            blocks = []
            for term in terms:
                wide = jnp.broadcast_to(term[here, :], (16, LANES)).astype(BF16)
                blocks.append(hot * jnp.concatenate([wide] * (half // 16), 0))
            left.append(jnp.concatenate(blocks, 0))
            right.append((col_ids == col[here, :]).astype(F32).astype(BF16))
            hots.append((slot_ids == slot[here, :]).astype(F32).astype(BF16))
            row_left.append(jnp.concatenate([term[here, :] for term in row_terms], 0))
        points = lax.dot_general(
            jnp.concatenate(left, 1), jnp.concatenate(right, 1), NT, preferred_element_type=F32
        )
        by_slot = lax.dot_general(
            jnp.concatenate(row_left, 1).astype(BF16), jnp.concatenate(hots, 1), NT,
            preferred_element_type=F32,
        )
        return points, by_slot

    points, by_slot = chunk(0)
    acc[...] = points
    row_acc[...] = by_slot

    @pl.loop(1, rows // step)
    def _(i):
        points, by_slot = chunk(pl.multiple_of(i * step, step))
        acc[...] += points
        row_acc[...] += by_slot


def kernel(
    n_region, n_member, members,
    ens_hbm, value_hbm, var_hbm, point_hbm, owned_hbm, pmean_hbm, pvar_hbm,
    out_ref, post_ref,
    ens, value, var, point, owned, pmean, pvar,
    part, rs_recv, means, factors, acc, row_acc, place, place_recv,
    in_sem, rs_send, rs_got, mean_send, mean_got, f_send, f_got, pl_send, pl_got,
):
    region = lax.axis_index("region")
    me = lax.axis_index("member")
    slots = owned.shape[1]
    own = slots // n_member
    half = slots // 2
    devices = n_region * n_member
    flat = region * n_member + me

    def device(i):
        there = lax.rem(flat + i, devices)
        return there, (there // n_member, lax.rem(there, n_member))

    def peer(i):
        return {"member": lax.rem(me + i, n_member)}

    barrier = pltpu.get_barrier_semaphore()
    for i in range(1, devices):
        pl.semaphore_signal(barrier, inc=1, device_id=device(i)[1], device_id_type=MESH)
    pairs = (
        (point_hbm, point), (value_hbm, value), (var_hbm, var), (ens_hbm, ens),
        (owned_hbm, owned), (pmean_hbm, pmean), (pvar_hbm, pvar),
    )
    loads = [pltpu.make_async_copy(s, d, in_sem.at[i]) for i, (s, d) in enumerate(pairs)]
    for load in loads:
        load.start()
    for load in loads[:3]:
        load.wait()
    scatter(value, var, point, acc, row_acc, half)

    for index, (first, last) in enumerate(((0, 1), (1, 3), (3, 5))):
        both = acc[first * half : (first + 1) * half, :]
        for other in range(first + 1, last):
            both = both + acc[other * half : (other + 1) * half, :]
        table = jnp.concatenate([both[:, :LANES], both[:, LANES:]], 0)
        for k in range(n_member):
            part[k, (2 + index) * own : (3 + index) * own, :] = table[k * own : (k + 1) * own]
    sums = row_acc[...]
    rows = jnp.concatenate(
        [
            sums[0:1] + sums[1:2],
            sums[2:3] + sums[3:4] + sums[4:5],
            sums[5:6] + sums[6:7] + sums[7:8],
            jnp.zeros((5, slots), F32),
        ],
        0,
    )
    for k in range(n_member):
        part[k, 5 * own :, :] = rows

    for load in loads[3:]:
        load.wait()

    @pl.loop(0, n_member)
    def _(k):
        @pl.loop(0, own, unroll=8)
        def _(r):
            start = pl.multiple_of((k * own + r) * LANES, LANES)
            wide = ens[:, pl.ds(start, LANES)].astype(F32)
            part[k, pl.ds(r, 1), :] = jnp.sum(wide, 0, keepdims=True)
            part[k, pl.ds(own + r, 1), :] = jnp.sum(wide * wide, 0, keepdims=True)

    pl.semaphore_wait(barrier, devices - 1)
    rs = []
    for i in range(1, n_member):
        copy = pltpu.make_async_remote_copy(
            part.at[lax.rem(me + i, n_member)], rs_recv.at[i], rs_send.at[i], rs_got.at[i],
            device_id=peer(i), device_id_type=MESH,
        )
        copy.start()
        rs.append(copy)

    block = owned[...]
    groups = pmean.shape[0]
    lane_hot = (
        lax.broadcasted_iota(jnp.int32, (LANES, slots), 0) == (block & (LANES - 1))
    ).astype(F32).astype(BF16)
    table = jnp.concatenate(split(pmean[...], 3) + split(pvar[...], 3), 0).astype(BF16)
    picked = jnp.dot(table, lane_hot, preferred_element_type=F32)
    in_group = lax.broadcasted_iota(jnp.int32, (groups, slots), 0) == (block >> 7)

    def pick(first):
        total = picked[first * groups : (first + 1) * groups]
        for i in (1, 2):
            total = total + picked[(first + i) * groups : (first + i + 1) * groups]
        return jnp.sum(jnp.where(in_group, total, 0.0), 0, keepdims=True)

    prior_mean, prior_var = pick(0), pick(3)
    share = groups * LANES // devices
    lane = lax.broadcasted_iota(jnp.int32, (1, slots), 1)
    target = lax.broadcasted_iota(jnp.int32, (devices, slots), 0) == jnp.where(
        lane // own == me, block // share, -1
    )
    spots = (
        lax.broadcasted_iota(jnp.int32, (LANES, slots), 0) == lax.rem(block, share)
    ).astype(F32).astype(BF16)
    mine = lax.broadcasted_iota(jnp.int32, (own, slots), 1) == (
        lax.broadcasted_iota(jnp.int32, (own, slots), 0) + own * me
    )

    for copy in rs:
        copy.wait_recv()

    def reduced(first, last):
        total = part[me, first:last, :]
        for i in range(1, n_member):
            total = total + rs_recv[i, first:last, :]
        return total

    both = reduced(0, 2 * own)
    mean = both[:own] / members
    means[me] = mean
    ag = []
    for i in range(1, n_member):
        copy = pltpu.make_async_remote_copy(
            means.at[me], means.at[me], mean_send.at[i], mean_got.at[i],
            device_id=peer(i), device_id_type=MESH,
        )
        copy.start()
        ag.append(copy)
    spread = (both[own:] - members * mean * mean) / (members - 1)
    count = reduced(2 * own, 3 * own)
    y_sum = reduced(3 * own, 4 * own)
    v_sum = reduced(4 * own, 5 * own)
    by_slot = reduced(5 * own, 5 * own + 8)

    def to_row(table):
        column = jnp.sum(table, axis=1, keepdims=True)
        return jnp.sum(jnp.where(mine, column, 0.0), axis=0, keepdims=True)

    seen = count * spread
    so, soo = by_slot[0:1], by_slot[1:2]
    sd = by_slot[2:3] + to_row(mean * (count * mean - 2.0 * y_sum))
    sp, spp, spo = to_row(seen), to_row(seen * spread), to_row(v_sum * spread)
    weight = 2.0 * prior_mean * prior_mean * (1.0 + spp) + 4.0 * prior_mean * spo + 2.0 * soo
    post = jnp.maximum(
        (prior_mean * weight + prior_var * sp * (sd - so)) / (weight + prior_var * sp * sp), 1.0
    )

    sent = jnp.concatenate([jnp.where(target, term, 0.0) for term in split(post, 3)], 0)
    placed = lax.dot_general(sent.astype(BF16), spots, NT, preferred_element_type=F32)
    placed = placed[:devices] + placed[devices : 2 * devices] + placed[2 * devices :]
    for d in range(devices):
        place[d] = placed[d : d + 1]
    column = jnp.sum(jnp.where(mine, post, 0.0), axis=1, keepdims=True)
    factors[me] = jnp.broadcast_to(jnp.sqrt(column), (own, LANES))
    out_copies = []
    for i in range(1, devices):
        there, coords = device(i)
        copy = pltpu.make_async_remote_copy(
            place.at[there], place_recv.at[i], pl_send.at[i], pl_got.at[i],
            device_id=coords, device_id_type=MESH,
        )
        copy.start()
        out_copies.append(copy)
    for i in range(1, n_member):
        copy = pltpu.make_async_remote_copy(
            factors.at[me], factors.at[me], f_send.at[i], f_got.at[i],
            device_id=peer(i), device_id_type=MESH,
        )
        copy.start()
        ag.append(copy)
    for copy in ag:
        copy.wait_recv()

    @pl.loop(0, n_member)
    def _(k):
        @pl.loop(0, own, unroll=8)
        def _(r):
            start = pl.multiple_of((k * own + r) * LANES, LANES)
            wide = ens[:, pl.ds(start, LANES)].astype(F32)
            at = means[k, pl.ds(r, 1), :]
            out_ref[:, pl.ds(start, LANES)] = (
                at + factors[k, pl.ds(r, 1), :] * (wide - at)
            ).astype(BF16)

    for copy in out_copies:
        copy.wait_recv()
    result = place[flat]
    for i in range(1, devices):
        result = result + place_recv[i]
    post_ref[...] = result[:, :share]
    for copy in rs + ag + out_copies:
        copy.wait_send()


def body(n_region, n_member, ensemble, obs_value, obs_var, obs_point, owned, infl_mean, infl_var):
    members = ensemble.shape[0] * n_member
    slots = owned.shape[0]
    own = slots // n_member
    blocks = infl_mean.shape[0]
    devices = n_region * n_member
    share = blocks // devices
    owned = owned.reshape(1, slots)
    infl_mean = infl_mean.reshape(-1, LANES)
    infl_var = infl_var.reshape(-1, LANES)
    operands = (ensemble, obs_value, obs_var, obs_point, owned, infl_mean, infl_var)
    dma = pltpu.SemaphoreType.DMA
    inflated, post = pl.pallas_call(
        functools.partial(kernel, n_region, n_member, members),
        out_shape=(
            jax.ShapeDtypeStruct(ensemble.shape, BF16),
            jax.ShapeDtypeStruct((1, share), F32),
        ),
        in_specs=[pl.BlockSpec(memory_space=pltpu.HBM)] * len(operands),
        out_specs=(
            pl.BlockSpec(memory_space=pltpu.VMEM),
            pl.BlockSpec(memory_space=pltpu.VMEM),
        ),
        scratch_shapes=[pltpu.VMEM(a.shape, a.dtype) for a in operands]
        + [
            pltpu.VMEM((n_member, 5 * own + 8, LANES), F32),
            pltpu.VMEM((n_member, 5 * own + 8, LANES), F32),
            pltpu.VMEM((n_member, own, LANES), F32),
            pltpu.VMEM((n_member, own, LANES), F32),
            pltpu.VMEM((5 * (slots // 2), 2 * LANES), F32),
            pltpu.VMEM((8, slots), F32),
            pltpu.VMEM((devices, 1, LANES), F32),
            pltpu.VMEM((devices, 1, LANES), F32),
            dma((len(operands),)),
            dma((n_member,)), dma((n_member,)),
            dma((n_member,)), dma((n_member,)),
            dma((n_member,)), dma((n_member,)),
            dma((devices,)), dma((devices,)),
        ],
        compiler_params=pltpu.CompilerParams(collective_id=0, has_side_effects=True),
    )(*operands)
    return inflated, post.reshape(share)


def solution(mesh):
    placed = (
        P("member", "region"),
        P(("region", "member"), None),
        P(("region", "member"), None),
        P(("region", "member"), None),
        P("region"),
        P(),
        P(),
    )
    return jax.shard_map(
        functools.partial(body, mesh.shape["region"], mesh.shape["member"]),
        mesh=mesh,
        in_specs=placed,
        out_specs=(P("member", "region"), P(("region", "member"))),
        check_vma=False,
    )
```

```python
import functools

import jax
import jax.numpy as jnp
from jax import lax
from jax.experimental import pallas as pl
from jax.experimental.pallas import tpu as pltpu
from jax.sharding import PartitionSpec as P

LANES = 128
MESH = pl.DeviceIdType.MESH
F32 = jnp.float32
BF16 = jnp.bfloat16
NT = (((1,), (1,)), ((), ()))


def split(value, parts):
    terms = []
    for _ in range(parts):
        term = value.astype(BF16).astype(F32)
        terms.append(term)
        value = value - term
    return terms


def scatter(value_ref, var_ref, point_ref, acc, row_acc, half, first_part):
    rows = point_ref.shape[0]
    step = 8
    low_ids = lax.broadcasted_iota(jnp.int32, (half, LANES), 0)
    col_ids = lax.broadcasted_iota(jnp.int32, (2 * LANES, LANES), 0)
    slot_ids = lax.broadcasted_iota(jnp.int32, (2 * half, LANES), 0)

    def chunk(first):
        point = point_ref[pl.ds(first, step), :]
        slot = point >> 7
        upper = (slot >= half).astype(jnp.int32)
        low = slot - half * upper
        col = (point & (LANES - 1)) + LANES * upper
        y = split(value_ref[pl.ds(first, step), :], 2)
        exact = y[0] + y[1]
        raw = var_ref[pl.ds(first, step), :]
        v = split(raw, 2)
        terms = [jnp.ones_like(raw)] + y + v
        row_terms = v + split(raw * raw, 3) + split(exact * exact, 3)
        left, right, hots = [], [], []
        row_left = []
        for r in range(step):
            here = slice(r, r + 1)
            hot = (low_ids == low[here, :]).astype(F32).astype(BF16)
            blocks = []
            for term in terms:
                wide = jnp.broadcast_to(term[here, :], (16, LANES)).astype(BF16)
                blocks.append(hot * jnp.concatenate([wide] * (half // 16), 0))
            left.append(jnp.concatenate(blocks, 0))
            right.append((col_ids == col[here, :]).astype(F32).astype(BF16))
            hots.append((slot_ids == slot[here, :]).astype(F32).astype(BF16))
            row_left.append(jnp.concatenate([term[here, :] for term in row_terms], 0))
        points = lax.dot_general(
            jnp.concatenate(left, 1), jnp.concatenate(right, 1), NT, preferred_element_type=F32
        )
        by_slot = lax.dot_general(
            jnp.concatenate(row_left, 1).astype(BF16), jnp.concatenate(hots, 1), NT,
            preferred_element_type=F32,
        )
        return points, by_slot

    def add(i):
        points, by_slot = chunk(pl.multiple_of(i * step, step))
        acc[...] += points
        row_acc[...] += by_slot

    if first_part:
        points, by_slot = chunk(0)
        acc[...] = points
        row_acc[...] = by_slot
        pl.loop(1, rows // step // 2)(add)
    else:
        pl.loop(rows // step // 2, rows // step)(add)


def kernel(
    n_region, n_member, members,
    ens_hbm, value_hbm, var_hbm, point_hbm, owned_hbm, pmean_hbm, pvar_hbm,
    out_ref, post_ref,
    ens, value, var, point, owned, pmean, pvar,
    part, rs_recv, means, factors, acc, row_acc, place, place_recv,
    in_sem, rs_send, rs_got, mean_send, mean_got, f_send, f_got, pl_send, pl_got,
):
    region = lax.axis_index("region")
    me = lax.axis_index("member")
    slots = owned.shape[1]
    own = slots // n_member
    half = slots // 2
    devices = n_region * n_member
    flat = region * n_member + me

    def device(i):
        there = lax.rem(flat + i, devices)
        return there, (there // n_member, lax.rem(there, n_member))

    def peer(i):
        return {"member": lax.rem(me + i, n_member)}

    barrier = pltpu.get_barrier_semaphore()
    for i in range(1, devices):
        pl.semaphore_signal(barrier, inc=1, device_id=device(i)[1], device_id_type=MESH)
    pairs = (
        (ens_hbm, ens), (point_hbm, point), (value_hbm, value), (var_hbm, var),
        (owned_hbm, owned), (pmean_hbm, pmean), (pvar_hbm, pvar),
    )
    loads = [pltpu.make_async_copy(s, d, in_sem.at[i]) for i, (s, d) in enumerate(pairs)]
    for load in loads:
        load.start()
    loads[0].wait()

    @pl.loop(0, n_member)
    def _(k):
        @pl.loop(0, own, unroll=8)
        def _(r):
            start = pl.multiple_of((k * own + r) * LANES, LANES)
            wide = ens[:, pl.ds(start, LANES)].astype(F32)
            part[k, pl.ds(r, 1), :] = jnp.sum(wide, 0, keepdims=True)
            part[k, pl.ds(own + r, 1), :] = jnp.sum(wide * wide, 0, keepdims=True)

    for load in loads[1:]:
        load.wait()
    scatter(value, var, point, acc, row_acc, half, True)
    pl.semaphore_wait(barrier, devices - 1)

    def reduce_copies(first, count, which):
        copies = []
        for i in range(1, n_member):
            copy = pltpu.make_async_remote_copy(
                part.at[lax.rem(me + i, n_member), pl.ds(first, count), :],
                rs_recv.at[i, pl.ds(first, count), :],
                rs_send.at[which, i], rs_got.at[which, i],
                device_id=peer(i), device_id_type=MESH,
            )
            copy.start()
            copies.append(copy)
        return copies

    rs = reduce_copies(0, 2 * own, 0)
    scatter(value, var, point, acc, row_acc, half, False)

    for index, (first, last) in enumerate(((0, 1), (1, 3), (3, 5))):
        both = acc[first * half : (first + 1) * half, :]
        for other in range(first + 1, last):
            both = both + acc[other * half : (other + 1) * half, :]
        table = jnp.concatenate([both[:, :LANES], both[:, LANES:]], 0)
        for k in range(n_member):
            part[k, (2 + index) * own : (3 + index) * own, :] = table[k * own : (k + 1) * own]
    sums = row_acc[...]
    rows = jnp.concatenate(
        [
            sums[0:1] + sums[1:2],
            sums[2:3] + sums[3:4] + sums[4:5],
            sums[5:6] + sums[6:7] + sums[7:8],
            jnp.zeros((5, slots), F32),
        ],
        0,
    )
    for k in range(n_member):
        part[k, 5 * own :, :] = rows

    rs_rest = reduce_copies(2 * own, 3 * own + 8, 1)

    block = owned[...]
    groups = pmean.shape[0]
    lane_hot = (
        lax.broadcasted_iota(jnp.int32, (LANES, slots), 0) == (block & (LANES - 1))
    ).astype(F32).astype(BF16)
    table = jnp.concatenate(split(pmean[...], 3) + split(pvar[...], 3), 0).astype(BF16)
    picked = jnp.dot(table, lane_hot, preferred_element_type=F32)
    in_group = lax.broadcasted_iota(jnp.int32, (groups, slots), 0) == (block >> 7)

    def pick(first):
        total = picked[first * groups : (first + 1) * groups]
        for i in (1, 2):
            total = total + picked[(first + i) * groups : (first + i + 1) * groups]
        return jnp.sum(jnp.where(in_group, total, 0.0), 0, keepdims=True)

    prior_mean, prior_var = pick(0), pick(3)
    share = groups * LANES // devices
    lane = lax.broadcasted_iota(jnp.int32, (1, slots), 1)
    target = lax.broadcasted_iota(jnp.int32, (devices, slots), 0) == jnp.where(
        lane // own == me, block // share, -1
    )
    spots = (
        lax.broadcasted_iota(jnp.int32, (LANES, slots), 0) == lax.rem(block, share)
    ).astype(F32).astype(BF16)
    mine = lax.broadcasted_iota(jnp.int32, (own, slots), 1) == (
        lax.broadcasted_iota(jnp.int32, (own, slots), 0) + own * me
    )

    for copy in rs:
        copy.wait_recv()

    def reduced(first, last):
        total = part[me, first:last, :]
        for i in range(1, n_member):
            total = total + rs_recv[i, first:last, :]
        return total

    both = reduced(0, 2 * own)
    mean = both[:own] / members
    means[me] = mean
    ag = []
    for i in range(1, n_member):
        copy = pltpu.make_async_remote_copy(
            means.at[me], means.at[me], mean_send.at[i], mean_got.at[i],
            device_id=peer(i), device_id_type=MESH,
        )
        copy.start()
        ag.append(copy)
    spread = (both[own:] - members * mean * mean) / (members - 1)
    for copy in rs_rest:
        copy.wait_recv()
    count = reduced(2 * own, 3 * own)
    y_sum = reduced(3 * own, 4 * own)
    v_sum = reduced(4 * own, 5 * own)
    by_slot = reduced(5 * own, 5 * own + 8)

    def to_row(table):
        column = jnp.sum(table, axis=1, keepdims=True)
        return jnp.sum(jnp.where(mine, column, 0.0), axis=0, keepdims=True)

    seen = count * spread
    so, soo = by_slot[0:1], by_slot[1:2]
    sd = by_slot[2:3] + to_row(mean * (count * mean - 2.0 * y_sum))
    sp, spp, spo = to_row(seen), to_row(seen * spread), to_row(v_sum * spread)
    weight = 2.0 * prior_mean * prior_mean * (1.0 + spp) + 4.0 * prior_mean * spo + 2.0 * soo
    post = jnp.maximum(
        (prior_mean * weight + prior_var * sp * (sd - so)) / (weight + prior_var * sp * sp), 1.0
    )

    sent = jnp.concatenate([jnp.where(target, term, 0.0) for term in split(post, 3)], 0)
    placed = lax.dot_general(sent.astype(BF16), spots, NT, preferred_element_type=F32)
    placed = placed[:devices] + placed[devices : 2 * devices] + placed[2 * devices :]
    for d in range(devices):
        place[d] = placed[d : d + 1]
    column = jnp.sum(jnp.where(mine, post, 0.0), axis=1, keepdims=True)
    factors[me] = jnp.broadcast_to(jnp.sqrt(column), (own, LANES))
    out_copies = []
    for i in range(1, devices):
        there, coords = device(i)
        copy = pltpu.make_async_remote_copy(
            place.at[there], place_recv.at[i], pl_send.at[i], pl_got.at[i],
            device_id=coords, device_id_type=MESH,
        )
        copy.start()
        out_copies.append(copy)
    for i in range(1, n_member):
        copy = pltpu.make_async_remote_copy(
            factors.at[me], factors.at[me], f_send.at[i], f_got.at[i],
            device_id=peer(i), device_id_type=MESH,
        )
        copy.start()
        ag.append(copy)
    for copy in ag:
        copy.wait_recv()

    @pl.loop(0, n_member)
    def _(k):
        @pl.loop(0, own, unroll=8)
        def _(r):
            start = pl.multiple_of((k * own + r) * LANES, LANES)
            wide = ens[:, pl.ds(start, LANES)].astype(F32)
            at = means[k, pl.ds(r, 1), :]
            out_ref[:, pl.ds(start, LANES)] = (
                at + factors[k, pl.ds(r, 1), :] * (wide - at)
            ).astype(BF16)

    for copy in out_copies:
        copy.wait_recv()
    result = place[flat]
    for i in range(1, devices):
        result = result + place_recv[i]
    post_ref[...] = result[:, :share]
    for copy in rs + rs_rest + ag + out_copies:
        copy.wait_send()


def body(n_region, n_member, ensemble, obs_value, obs_var, obs_point, owned, infl_mean, infl_var):
    members = ensemble.shape[0] * n_member
    slots = owned.shape[0]
    own = slots // n_member
    blocks = infl_mean.shape[0]
    devices = n_region * n_member
    share = blocks // devices
    owned = owned.reshape(1, slots)
    infl_mean = infl_mean.reshape(-1, LANES)
    infl_var = infl_var.reshape(-1, LANES)
    operands = (ensemble, obs_value, obs_var, obs_point, owned, infl_mean, infl_var)
    dma = pltpu.SemaphoreType.DMA
    operands = tuple(pltpu.with_memory_space_constraint(x, pltpu.HBM) for x in operands)
    inflated, post = pl.pallas_call(
        functools.partial(kernel, n_region, n_member, members),
        out_shape=(
            jax.ShapeDtypeStruct(ensemble.shape, BF16),
            jax.ShapeDtypeStruct((1, share), F32),
        ),
        in_specs=[pl.BlockSpec(memory_space=pltpu.HBM)] * len(operands),
        out_specs=(
            pl.BlockSpec(memory_space=pltpu.VMEM),
            pl.BlockSpec(memory_space=pltpu.VMEM),
        ),
        scratch_shapes=[pltpu.VMEM(a.shape, a.dtype) for a in operands]
        + [
            pltpu.VMEM((n_member, 5 * own + 8, LANES), F32),
            pltpu.VMEM((n_member, 5 * own + 8, LANES), F32),
            pltpu.VMEM((n_member, own, LANES), F32),
            pltpu.VMEM((n_member, own, LANES), F32),
            pltpu.VMEM((5 * (slots // 2), 2 * LANES), F32),
            pltpu.VMEM((8, slots), F32),
            pltpu.VMEM((devices, 1, LANES), F32),
            pltpu.VMEM((devices, 1, LANES), F32),
            dma((len(operands),)),
            dma((2, n_member)), dma((2, n_member)),
            dma((n_member,)), dma((n_member,)),
            dma((n_member,)), dma((n_member,)),
            dma((devices,)), dma((devices,)),
        ],
        compiler_params=pltpu.CompilerParams(collective_id=0, has_side_effects=True, vmem_limit_bytes=12*2**20),
    )(*operands)
    return inflated, post.reshape(share)


def solution(mesh):
    placed = (
        P("member", "region"),
        P(("region", "member"), None),
        P(("region", "member"), None),
        P(("region", "member"), None),
        P("region"),
        P(),
        P(),
    )
    return jax.shard_map(
        functools.partial(body, mesh.shape["region"], mesh.shape["member"]),
        mesh=mesh,
        in_specs=placed,
        out_specs=(P("member", "region"), P(("region", "member"))),
        check_vma=False,
    )
```
